16 devices in a mesh: batch: 2 (over y, z), row: 8 (over x, core).
Axes of the slice: x: 4, y: 2, z: 1, core: 2. Of those that a mesh axis runs over, the one named last changes fastest.
The devices are a block of a 4x4x8 slice.
Arguments:
- trans_mat: bfloat16 [32768, 16384], P(('batch', 'row')), parts along dimension 0
- teleport: float32 [32768, 128], P(('batch', 'row')), parts along dimension 0
- dangling: int32 [32768], P(('batch', 'row')), parts along dimension 0
- damping: float32 [16], replicated
- rank_init: float32 [32768, 128], P(('batch', 'row')), parts along dimension 0
Outputs:
- output: float32 [32768, 128], P(('batch', 'row')), parts along dimension 0
There are 2 independent parts. The reference program is written for one: setup_inputs(seed, part) draws one part's arguments, and reference() takes and returns one part's arrays. A program takes and returns all parts, laid end to end along the dimension named above; an argument that names none is the same for every part.
All inputs are finite; a program needn't handle non-finite values.
Results may differ from the reference program's by a relative error of at most 0.001.
Values are sent between devices in bfloat16 or wider.
A program may use at most 768 MiB of HBM per device.

```python
import jax
import jax.numpy as jnp
from jax import lax

NODES = 16384
SEEDS = 128
SWEEPS = 16


def setup_inputs(seed: int = 0, part: int = 0) -> dict:
    base_key = jax.random.key(seed)
    part_key = jax.random.fold_in(base_key, part)
    key_list = jax.random.split(part_key, 8)
    dangling = (jax.random.randint(key_list[0], (NODES,), 0, 100) < 20).astype(jnp.int32)
    popular = jnp.exp(0.8 * jax.random.normal(key_list[1], (NODES,), jnp.float32))
    weights = popular[:, None] * jnp.maximum(jax.random.uniform(key_list[2], (NODES, NODES), jnp.float32) - 0.5, 0.0)
    keep_cols = 1.0 - dangling.astype(jnp.float32)
    col_sum = jnp.sum(weights, axis=0)
    trans_mat = (weights * (keep_cols / jnp.maximum(col_sum, 1e-6))[None, :]).astype(jnp.bfloat16)
    tele_raw = jnp.exp(1.2 * jax.random.normal(key_list[3], (NODES, SEEDS), jnp.float32))
    teleport = tele_raw / jnp.mean(tele_raw, axis=0, keepdims=True)
    col_scale = jax.random.uniform(key_list[4], (1, SEEDS), jnp.float32, 0.3, 3.0)
    rank_init = col_scale * jax.random.uniform(key_list[5], (NODES, SEEDS), jnp.float32, 0.2, 1.8)
    damping = jax.random.uniform(jax.random.key(seed + 1), (SWEEPS,), jnp.float32, 0.75, 0.95)
    return {"trans_mat": trans_mat, "teleport": teleport, "dangling": dangling, "damping": damping, "rank_init": rank_init}


def reference(trans_mat, teleport, dangling, damping, rank_init):
    dang_float = dangling.astype(jnp.float32)

    def one_sweep(rank_cur, factor):
        prod_rows = jnp.dot(trans_mat, rank_cur.astype(jnp.bfloat16), preferred_element_type=jnp.float32)
        dang_mass = jnp.dot(dang_float, rank_cur, preferred_element_type=jnp.float32)
        rank_next = factor * prod_rows + (1.0 - factor) * teleport + (factor / NODES) * dang_mass[None, :]
        return rank_next, None

    rank_final, unused = lax.scan(one_sweep, rank_init, damping)
    return rank_final
```

```python
import functools

import jax
import jax.numpy as jnp
from jax import lax
from jax.experimental import pallas as pl
from jax.experimental.pallas import tpu as pltpu
from jax.sharding import PartitionSpec as P

MESH = pl.DeviceIdType.MESH
TILE = 256
HALVES = 2
VMEM_LIMIT = 67043328


def acc_specs(halves, tiles, rows):
    return [[pltpu.VMEM((rows, TILE), jnp.float32) for i in range(tiles)] for _ in range(halves)]


def acc_add(accs, halves, tile, count, lhs, rhs, flip):
    for i, h in enumerate(halves):
        accs[h][tile][...] += lax.dot_general(lhs[i], rhs, (((1,), (1 if flip else 0,)), ((), ())), preferred_element_type=jnp.float32)


def acc_pop(acc):
    v = acc[...]
    acc[...] = jnp.zeros_like(v)
    return v


def sweeps_kernel(n, num_sweeps, num_nodes, dang, damp, a3, e3, r3, out3, cache, gath, stream, et, rst, mcol, pm, part,
                  recv_l, recv_r, sib_own, sib_l, sib_r, send_sem, m_recv, m_send, c_sem, s_sem, io_sem):
    tiles = a3.shape[0]
    pieces, seeds, width = gath.shape[3], gath.shape[4], gath.shape[5]
    kts = width // TILE
    block = pieces * width
    pair = pieces // 2
    chunks = block // TILE
    bufs = stream.shape[0]
    lanes = et.shape[2]
    per_tile = TILE // lanes

    me = lax.axis_index("row")
    step = 1 - 2 * lax.rem(me, 2)
    sib = me + step
    right, left, opp = lax.rem(me + 2, n), lax.rem(me + n - 2, n), lax.rem(me + n // 2, n)

    def piece(slot, blk, h, p, count):
        return gath.at[slot, blk, h, pl.ds(p, count)]

    def remote(slot, blk, h, p, count, recv, dev):
        ref = piece(slot, blk, h, p, count)
        return pltpu.make_async_remote_copy(src_ref=ref, dst_ref=ref, send_sem=send_sem.at[slot], recv_sem=recv,
                                            device_id={"row": dev}, device_id_type=MESH)

    def send(*args):
        remote(*args).start()

    def arrive(slot, blk, h, p, count, recv):
        remote(slot, blk, h, p, count, recv, sib).wait_recv()

    def wait_sends(slot):
        ref = gath.at[slot, pl.ds(0, n - 1)]
        pltpu.make_async_copy(ref, ref, send_sem.at[slot]).wait()

    def others(fn):
        for k in range(1, n):
            fn(lax.rem(me + k, n))

    def stream_copy(c):
        blk = me + (c // chunks) * (sib - me)
        col = pl.multiple_of(blk * block + lax.rem(c, chunks) * TILE, TILE)
        b = lax.rem(c, bufs)
        return pltpu.make_async_copy(a3.at[:, :, pl.ds(col, TILE)], stream.at[b], s_sem.at[b])

    def cache_copy(ci, kt, blk, p):
        col = pl.multiple_of(blk * block + p * width + kt * TILE, TILE)
        return pltpu.make_async_copy(a3.at[:, :, pl.ds(col, TILE)], cache.at[ci, kt], c_sem.at[ci, kt])

    blocks = [left, right, left + step, right + step, opp, opp + step]

    def entry(accs):
        barrier = pltpu.get_barrier_semaphore()
        others(lambda dev: pl.semaphore_signal(barrier, inc=1, device_id={"row": dev}, device_id_type=MESH))
        load_r = pltpu.make_async_copy(r3, rst, io_sem.at[0])
        load_e = pltpu.make_async_copy(e3, et, io_sem.at[1])
        load_r.start()
        load_e.start()
        for c in range(bufs):
            stream_copy(c).start()

        def start_cache(b, p):
            for kt in range(kts):
                cache_copy(b * pieces + p, kt, blocks[b], p).start()

        for i in range(2):
            for b in range(4):
                for j in range(pair):
                    start_cache(b, (i if b % 2 == 0 else 1 - i) * pair + j)
        for b in (4, 5):
            for j in range(pair):
                start_cache(b, j)
                start_cache(b, pair + j)
        for h in range(HALVES):
            for i in range(tiles):
                acc_pop(accs[h][i])

        def send_own(slot, h, u):
            if u == 0:
                send(slot, me, h, 0, pair, recv_l.at[slot, 2 * h], right)
                send(slot, me, h, 0, pair, sib_own.at[slot, 2 * h], sib)
            else:
                send(slot, me, h, pair, pair, recv_r.at[slot, 2 * h], left)
                send(slot, me, h, pair, pair, recv_l.at[slot, 2 * h + 1], right)
                send(slot, me, h, 0, pair, recv_r.at[slot, 2 * h + 1], left)
                send(slot, me, h, pair, pair, sib_own.at[slot, 2 * h + 1], sib)

        def pm_copy(slot, dev):
            return pltpu.make_async_remote_copy(src_ref=pm.at[slot, me], dst_ref=pm.at[slot, me], send_sem=m_send.at[slot],
                                                recv_sem=m_recv.at[slot], device_id={"row": dev}, device_id_type=MESH)

        def send_mass(slot):
            mass = jnp.sum(part[...], axis=1, keepdims=True)
            pm[slot, me] = jnp.transpose(jnp.broadcast_to(mass, (HALVES * seeds, lanes)))[: pm.shape[2]]
            others(lambda dev: pm_copy(slot, dev).start())

        def wait_mass(slot):
            ref = pm.at[slot, pl.ds(0, n - 1)]
            pltpu.make_async_copy(ref, ref, m_recv.at[slot]).wait()
            pltpu.make_async_copy(ref, ref, m_send.at[slot]).wait()

        def put(slot, h, j, val):
            p, off = j * lanes // width, j * lanes % width
            gath[slot, me, h, p, :, off : off + lanes] = val.astype(jnp.bfloat16)
            rst[j, h * seeds : (h + 1) * seeds, :] = val
            return val * dang[j : j + 1, :].astype(jnp.float32)

        node_tiles = block // lanes

        load_r.wait()
        pl.semaphore_wait(barrier, n - 1)
        for j in range(node_tiles):
            rst[j] = jnp.transpose(rst[j])
        for h in range(HALVES):
            total = jnp.zeros((seeds, lanes), jnp.float32)
            for j in range(node_tiles):
                total += put(0, h, j, rst[j, h * seeds : (h + 1) * seeds, :])
                if j == node_tiles // 2 - 1:
                    send_own(0, h, 0)
            send_own(0, h, 1)
            part[h * seeds : (h + 1) * seeds, :] = total
        send_mass(0)
        load_e.wait()
        for j in range(node_tiles):
            et[j] = jnp.transpose(et[j])

        def compute(first, slot, items, halves):
            count = 0
            for b, p in items:
                lhs = [gath[slot, blocks[b], h, p] for h in halves]
                for kt in range(kts):
                    if first:
                        cache_copy(b * pieces + p, kt, blocks[b], p).wait()
                    cut = [v[:, kt * TILE : (kt + 1) * TILE] for v in lhs]
                    for i in range(tiles):
                        rhs = cache[b * pieces + p, kt, i]
                        if first:
                            rhs = jnp.transpose(rhs)
                            cache[b * pieces + p, kt, i] = rhs
                        acc_add(accs, halves, i, count + i // 2, cut, rhs, False)
                    count += tiles // 2

        def near(slot, blk, base):
            def trip(i, carry):
                count = 0
                for j in range(bufs):
                    c = base + i * bufs + j
                    p = i * (bufs // kts) + j // kts
                    stream_copy(c).wait()
                    cut = [gath[slot, blk, h, p, :, (j % kts) * TILE : (j % kts + 1) * TILE] for h in range(HALVES)]
                    for k in range(tiles):
                        acc_add(accs, range(HALVES), k, count + k // 2, cut, stream[j, k], True)
                    count += tiles // 2
                    stream_copy(lax.rem(c + bufs, 2 * chunks)).start()
                return carry

            lax.fori_loop(0, chunks // bufs, trip, 0)

        def finish(t, slot, h):
            nxt = 1 - slot
            factor = damp[t]
            rows = slice(h * seeds, (h + 1) * seeds)
            total = jnp.zeros((seeds, lanes), jnp.float32)
            mass = mcol[rows, :] * (factor / num_nodes)
            for i in range(tiles):
                prod = acc_pop(accs[h][i])
                for k in range(per_tile):
                    j = i * per_tile + k
                    val = factor * prod[:, k * lanes : (k + 1) * lanes] + (1.0 - factor) * et[j, rows, :] + mass
                    total += put(nxt, h, j, val)
                if i == tiles // 2 - 1:
                    pl.when(t < num_sweeps - 1)(lambda: send_own(nxt, h, 0))
            pl.when(t < num_sweeps - 1)(lambda: send_own(nxt, h, 1))
            part[rows, :] = total

        def sweep(t, slot, first):
            near(slot, me, 0)
            for h in range(HALVES):
                for u in range(2):
                    arrive(slot, sib, h, u * pair, pair, sib_own.at[slot, 2 * h + u])
            near(slot, sib, chunks)
            if not first:
                wait_sends(1 - slot)

            def pass_on(h, i):
                arrive(slot, left, h, i * pair, pair, recv_l.at[slot, 2 * h + i])
                if i == 0:
                    for j in range(pair):
                        send(slot, left, h, j, 1, recv_l.at[slot, 4 + 2 * h + j], right)
                arrive(slot, right, h, (1 - i) * pair, pair, recv_r.at[slot, 2 * h + i])
                if i == 0:
                    for j in range(pair):
                        send(slot, right, h, pair + j, 1, recv_r.at[slot, 4 + 2 * h + j], left)
                send(slot, left, h, i * pair, pair, sib_l.at[slot, 2 * h + i], sib)
                send(slot, right, h, (1 - i) * pair, pair, sib_r.at[slot, 2 * h + i], sib)

            pass_on(0, 0)
            pass_on(0, 1)
            for i in range(2):
                pass_on(1, i)

                def direct(j, carry):
                    compute(first, slot, [(0, i * pair + j), (1, (1 - i) * pair + j)], range(HALVES))
                    return carry

                lax.fori_loop(0, pair, direct, 0)
                for h in range(HALVES):
                    arrive(slot, blocks[2], h, i * pair, pair, sib_l.at[slot, 2 * h + i])
                    arrive(slot, blocks[3], h, (1 - i) * pair, pair, sib_r.at[slot, 2 * h + i])

                def through(j, carry):
                    compute(first, slot, [(2, i * pair + j), (3, (1 - i) * pair + j)], range(HALVES))
                    return carry

                lax.fori_loop(0, pair, through, 0)

            wait_mass(slot)
            row = jnp.sum(pm[slot], axis=0)[0:1]
            mcol[...] = jnp.transpose(jnp.broadcast_to(row, (lanes, HALVES * seeds)))
            for h in range(HALVES):

                def direct(j, carry):
                    k = 4 + 2 * h + j
                    arrive(slot, opp, h, j, 1, recv_l.at[slot, k])
                    send(slot, opp, h, j, 1, sib_l.at[slot, k], sib)
                    arrive(slot, opp, h, pair + j, 1, recv_r.at[slot, k])
                    send(slot, opp, h, pair + j, 1, sib_r.at[slot, k], sib)
                    compute(first and h == 0, slot, [(4, j), (4, pair + j)], [h])
                    return carry

                lax.fori_loop(0, pair, direct, 0)

                def through(j, carry):
                    k = 4 + 2 * h + j
                    arrive(slot, blocks[5], h, j, 1, sib_l.at[slot, k])
                    arrive(slot, blocks[5], h, pair + j, 1, sib_r.at[slot, k])
                    compute(first and h == 0, slot, [(5, j), (5, pair + j)], [h])
                    return carry

                lax.fori_loop(0, pair, through, 0)
                finish(t, slot, h)
            pl.when(t < num_sweeps - 1)(lambda: send_mass(1 - slot))

        sweep(0, 0, True)

        def trip(t, carry):
            sweep(t, lax.rem(t, 2), False)
            return carry

        lax.fori_loop(1, num_sweeps, trip, 0)

        wait_sends((num_sweeps - 1) % 2)
        for c in range(bufs):
            stream_copy(c).wait()
        for j in range(node_tiles):
            rst[j] = jnp.transpose(rst[j])
        store = pltpu.make_async_copy(rst, out3, io_sem.at[0])
        store.start()
        store.wait()

    pl.run_scoped(entry, acc_specs(HALVES, tiles, seeds))


def solution(mesh):
    n = mesh.shape["row"]
    spec_rows = P(("batch", "row"), None)
    spec_vec = P(("batch", "row"))

    def local_sweeps(mat_rows, tele_rows, dang_rows, damping, start_rows):
        rows, num_nodes = mat_rows.shape
        num_seeds = start_rows.shape[1]
        lanes, width, bufs = 128, 512, 4
        assert n == 8 and rows * n == num_nodes and num_seeds == lanes
        tiles, pieces = rows // TILE, rows // width
        f32, bf16 = jnp.float32, jnp.bfloat16
        tile3 = (rows // lanes, lanes, num_seeds)
        dma, hbm = pltpu.SemaphoreType.DMA, pl.BlockSpec(memory_space=pl.ANY)
        out = pl.pallas_call(
            functools.partial(sweeps_kernel, n, damping.shape[0], num_nodes),
            out_shape=jax.ShapeDtypeStruct(tile3, f32),
            in_specs=[pl.BlockSpec(memory_space=pltpu.VMEM), pl.BlockSpec(memory_space=pltpu.SMEM), hbm, hbm, hbm],
            out_specs=hbm,
            scratch_shapes=[
                pltpu.VMEM(((n - 2) * pieces, width // TILE, tiles, TILE, TILE), bf16),
                pltpu.VMEM((2, n, HALVES, pieces, num_seeds // HALVES, width), bf16),
                pltpu.VMEM((bufs, tiles, TILE, TILE), bf16),
                pltpu.VMEM(tile3, f32),
                pltpu.VMEM(tile3, f32),
                pltpu.VMEM((num_seeds, lanes), f32),
                pltpu.VMEM((2, n, 8, lanes), f32),
                pltpu.VMEM((num_seeds, lanes), f32),
                dma((2, 8)), dma((2, 8)), dma((2, 4)), dma((2, 8)), dma((2, 8)),
                dma((2,)), dma((2,)), dma((2,)),
                dma(((n - 2) * pieces, width // TILE)), dma((bufs,)), dma((2,)),
            ],
            compiler_params=pltpu.CompilerParams(collective_id=0, has_side_effects=True, vmem_limit_bytes=VMEM_LIMIT),
        )(
            dang_rows.reshape(rows // lanes, lanes),
            damping,
            mat_rows.reshape(tiles, TILE, num_nodes),
            tele_rows.reshape(tile3),
            start_rows.reshape(tile3),
        )
        return out.reshape(rows, num_seeds)

    return jax.shard_map(local_sweeps, mesh=mesh, in_specs=(spec_rows, spec_rows, spec_vec, P(None), spec_rows), out_specs=spec_rows, check_vma=False)
```

```python
import functools

import jax
import jax.numpy as jnp
from jax import lax
from jax.experimental import pallas as pl
from jax.experimental.pallas import tpu as pltpu
from jax.sharding import PartitionSpec as P

MESH = pl.DeviceIdType.MESH
TILE = 256
HALVES = 2
VMEM_LIMIT = 67043328


def product(lhs, rhs, flip):
    return lax.dot_general(lhs, rhs, (((1,), (1 if flip else 0,)), ((), ())), preferred_element_type=jnp.float32)


def sweeps_kernel(n, num_sweeps, num_nodes, dang, damp, a3, e3, r3, out3, cache, gath, stream, et, acc, mcol, pm, part,
                  recv_l, recv_r, sib_own, sib_l, sib_r, send_sem, m_recv, m_send, c_sem, s_sem, io_sem):
    tiles = a3.shape[0]
    pieces, seeds, width = gath.shape[3], gath.shape[4], gath.shape[5]
    kts = width // TILE
    block = pieces * width
    pair = pieces // 2
    chunks = block // TILE
    bufs = stream.shape[0]
    lanes = et.shape[2]
    per_tile = TILE // lanes

    me = lax.axis_index("row")
    step = 1 - 2 * lax.rem(me, 2)
    sib = me + step
    right, left, opp = lax.rem(me + 2, n), lax.rem(me + n - 2, n), lax.rem(me + n // 2, n)

    def piece(slot, blk, h, p, count):
        return gath.at[slot, blk, h, pl.ds(p, count)]

    def remote(slot, blk, h, p, count, recv, dev):
        ref = piece(slot, blk, h, p, count)
        return pltpu.make_async_remote_copy(src_ref=ref, dst_ref=ref, send_sem=send_sem.at[slot], recv_sem=recv,
                                            device_id={"row": dev}, device_id_type=MESH)

    def send(*args):
        remote(*args).start()

    def arrive(slot, blk, h, p, count, recv):
        remote(slot, blk, h, p, count, recv, sib).wait_recv()

    def wait_sends(slot):
        ref = gath.at[slot, pl.ds(0, n - 1)]
        pltpu.make_async_copy(ref, ref, send_sem.at[slot]).wait()

    def others(fn):
        for k in range(1, n):
            fn(lax.rem(me + k, n))

    def stream_copy(c):
        blk = me + (c // chunks) * (sib - me)
        col = pl.multiple_of(blk * block + lax.rem(c, chunks) * TILE, TILE)
        b = lax.rem(c, bufs)
        return pltpu.make_async_copy(a3.at[:, :, pl.ds(col, TILE)], stream.at[b], s_sem.at[b])

    def cache_copy(ci, kt, blk, p):
        col = pl.multiple_of(blk * block + p * width + kt * TILE, TILE)
        return pltpu.make_async_copy(a3.at[:, :, pl.ds(col, TILE)], cache.at[ci, kt], c_sem.at[ci, kt])

    blocks = [left, right, left + step, right + step, opp, opp + step]

    def entry():
        barrier = pltpu.get_barrier_semaphore()
        others(lambda dev: pl.semaphore_signal(barrier, inc=1, device_id={"row": dev}, device_id_type=MESH))
        load_r = pltpu.make_async_copy(r3, acc, io_sem.at[0])
        load_e = pltpu.make_async_copy(e3, et, io_sem.at[1])
        load_r.start()
        load_e.start()
        for c in range(bufs):
            stream_copy(c).start()

        def load_cache():
            def start_cache(b, p):
                for kt in range(kts):
                    cache_copy(b * pieces + p, kt, blocks[b], p).start()

            for i in range(2):
                for b in range(4):
                    for j in range(pair):
                        start_cache(b, (i if b % 2 == 0 else 1 - i) * pair + j)
            for b in (4, 5):
                for j in range(pair):
                    start_cache(b, j)
                    start_cache(b, pair + j)

        def send_own(slot, h, u):
            if u == 0:
                send(slot, me, h, 0, pair, recv_l.at[slot, 2 * h], right)
                send(slot, me, h, 0, pair, sib_own.at[slot, 2 * h], sib)
            else:
                send(slot, me, h, pair, pair, recv_r.at[slot, 2 * h], left)
                send(slot, me, h, pair, pair, recv_l.at[slot, 2 * h + 1], right)
                send(slot, me, h, 0, pair, recv_r.at[slot, 2 * h + 1], left)
                send(slot, me, h, pair, pair, sib_own.at[slot, 2 * h + 1], sib)

        def pm_copy(slot, dev):
            return pltpu.make_async_remote_copy(src_ref=pm.at[slot, me], dst_ref=pm.at[slot, me], send_sem=m_send.at[slot],
                                                recv_sem=m_recv.at[slot], device_id={"row": dev}, device_id_type=MESH)

        def send_mass(slot):
            mass = jnp.sum(part[...], axis=1, keepdims=True)
            pm[slot, me] = jnp.transpose(jnp.broadcast_to(mass, (HALVES * seeds, lanes)))[: pm.shape[2]]
            others(lambda dev: pm_copy(slot, dev).start())

        def wait_mass(slot):
            ref = pm.at[slot, pl.ds(0, n - 1)]
            pltpu.make_async_copy(ref, ref, m_recv.at[slot]).wait()
            pltpu.make_async_copy(ref, ref, m_send.at[slot]).wait()

        def put(slot, h, j, val):
            p, off = j * lanes // width, j * lanes % width
            gath[slot, me, h, p, :, off : off + lanes] = val.astype(jnp.bfloat16)
            acc[j, h * seeds : (h + 1) * seeds, :] = val
            return val * dang[j : j + 1, :].astype(jnp.float32)

        node_tiles = block // lanes

        load_r.wait()
        pl.semaphore_wait(barrier, n - 1)
        for j in range(node_tiles):
            acc[j] = jnp.transpose(acc[j])
        for h in range(HALVES):
            total = jnp.zeros((seeds, lanes), jnp.float32)
            for j in range(node_tiles):
                total += put(0, h, j, acc[j, h * seeds : (h + 1) * seeds, :])
                if j == node_tiles // 2 - 1:
                    send_own(0, h, 0)
            send_own(0, h, 1)
            part[h * seeds : (h + 1) * seeds, :] = total
        send_mass(0)
        load_e.wait()
        for j in range(node_tiles):
            et[j] = jnp.transpose(et[j])

        def add(i, rows, val, fresh):
            for k in range(per_tile):
                j = i * per_tile + k
                cut = val[:, k * lanes : (k + 1) * lanes]
                acc[j, rows, :] = cut if fresh else acc[j, rows, :] + cut

        def left_side(slot, blk, halves, p, kt):
            cuts = [gath[slot, blk, h, p, :, kt * TILE : (kt + 1) * TILE] for h in halves]
            return cuts[0] if len(cuts) == 1 else jnp.concatenate(cuts, axis=0)

        def compute(first, slot, items, halves):
            rows = slice(halves[0] * seeds, (halves[-1] + 1) * seeds)
            if first:
                for b, p in items:
                    for kt in range(kts):
                        cache_copy(b * pieces + p, kt, blocks[b], p).wait()
            for i in range(tiles):
                val = None
                for b, p in items:
                    for kt in range(kts):
                        rhs = cache[b * pieces + p, kt, i]
                        if first:
                            rhs = jnp.transpose(rhs)
                            cache[b * pieces + p, kt, i] = rhs
                        term = product(left_side(slot, blocks[b], halves, p, kt), rhs, False)
                        val = term if val is None else val + term
                add(i, rows, val, False)

        def near(slot, blk, base):
            rows = slice(0, HALVES * seeds)

            def chunk(i, j, fresh):
                c = base + i * bufs + j
                p = i * (bufs // kts) + j // kts
                stream_copy(c).wait()
                lhs = left_side(slot, blk, range(HALVES), p, j % kts)
                for k in range(tiles):
                    add(k, rows, product(lhs, stream[j, k], True), fresh)
                stream_copy(lax.rem(c + bufs, 2 * chunks)).start()

            def trip(i, carry):
                for j in range(bufs):
                    chunk(i, j, False)
                return carry

            if base == 0:
                for j in range(bufs):
                    chunk(0, j, j == 0)
            lax.fori_loop(1 if base == 0 else 0, chunks // bufs, trip, 0)

        def finish(t, slot, h):
            nxt = 1 - slot
            factor = damp[t]
            rows = slice(h * seeds, (h + 1) * seeds)
            total = jnp.zeros((seeds, lanes), jnp.float32)
            mass = mcol[rows, :] * (factor / num_nodes)
            for i in range(tiles):
                for k in range(per_tile):
                    j = i * per_tile + k
                    val = factor * acc[j, rows, :] + (1.0 - factor) * et[j, rows, :] + mass
                    total += put(nxt, h, j, val)
                if i == tiles // 2 - 1:
                    pl.when(t < num_sweeps - 1)(lambda: send_own(nxt, h, 0))
            pl.when(t < num_sweeps - 1)(lambda: send_own(nxt, h, 1))
            part[rows, :] = total

        def sweep(t, slot, first):
            near(slot, me, 0)
            for h in range(HALVES):
                for u in range(2):
                    arrive(slot, sib, h, u * pair, pair, sib_own.at[slot, 2 * h + u])
            near(slot, sib, chunks)
            if first:
                load_cache()
            else:
                wait_sends(1 - slot)

            def pass_on(h, i):
                arrive(slot, left, h, i * pair, pair, recv_l.at[slot, 2 * h + i])
                if i == 0:
                    for j in range(pair):
                        send(slot, left, h, j, 1, recv_l.at[slot, 4 + 2 * h + j], right)
                arrive(slot, right, h, (1 - i) * pair, pair, recv_r.at[slot, 2 * h + i])
                if i == 0:
                    for j in range(pair):
                        send(slot, right, h, pair + j, 1, recv_r.at[slot, 4 + 2 * h + j], left)
                send(slot, left, h, i * pair, pair, sib_l.at[slot, 2 * h + i], sib)
                send(slot, right, h, (1 - i) * pair, pair, sib_r.at[slot, 2 * h + i], sib)

            pass_on(0, 0)
            pass_on(0, 1)
            for i in range(2):
                pass_on(1, i)
                compute(first, slot, [(b, (i if b == 0 else 1 - i) * pair + j) for b in (0, 1) for j in range(pair)], range(HALVES))
                for h in range(HALVES):
                    arrive(slot, blocks[2], h, i * pair, pair, sib_l.at[slot, 2 * h + i])
                    arrive(slot, blocks[3], h, (1 - i) * pair, pair, sib_r.at[slot, 2 * h + i])
                compute(first, slot, [(b, (i if b == 2 else 1 - i) * pair + j) for b in (2, 3) for j in range(pair)], range(HALVES))

            wait_mass(slot)
            row = jnp.sum(pm[slot], axis=0)[0:1]
            mcol[...] = jnp.transpose(jnp.broadcast_to(row, (lanes, HALVES * seeds)))
            for h in range(HALVES):

                def direct(j, carry):
                    k = 4 + 2 * h + j
                    arrive(slot, opp, h, j, 1, recv_l.at[slot, k])
                    send(slot, opp, h, j, 1, sib_l.at[slot, k], sib)
                    arrive(slot, opp, h, pair + j, 1, recv_r.at[slot, k])
                    send(slot, opp, h, pair + j, 1, sib_r.at[slot, k], sib)
                    compute(first and h == 0, slot, [(4, j), (4, pair + j)], [h])
                    return carry

                lax.fori_loop(0, pair, direct, 0)

                def through(j, carry):
                    k = 4 + 2 * h + j
                    arrive(slot, blocks[5], h, j, 1, sib_l.at[slot, k])
                    arrive(slot, blocks[5], h, pair + j, 1, sib_r.at[slot, k])
                    compute(first and h == 0, slot, [(5, j), (5, pair + j)], [h])
                    return carry

                lax.fori_loop(0, pair, through, 0)
                finish(t, slot, h)
            pl.when(t < num_sweeps - 1)(lambda: send_mass(1 - slot))

        sweep(0, 0, True)

        def trip(t, carry):
            sweep(t, lax.rem(t, 2), False)
            return carry

        lax.fori_loop(1, num_sweeps, trip, 0)

        wait_sends((num_sweeps - 1) % 2)
        for c in range(bufs):
            stream_copy(c).wait()
        for j in range(node_tiles):
            acc[j] = jnp.transpose(acc[j])
        store = pltpu.make_async_copy(acc, out3, io_sem.at[0])
        store.start()
        store.wait()

    entry()


def solution(mesh):
    n = mesh.shape["row"]
    spec_rows = P(("batch", "row"), None)
    spec_vec = P(("batch", "row"))

    def local_sweeps(mat_rows, tele_rows, dang_rows, damping, start_rows):
        rows, num_nodes = mat_rows.shape
        num_seeds = start_rows.shape[1]
        lanes, width, bufs = 128, 512, 4
        assert n == 8 and rows * n == num_nodes and num_seeds == lanes
        tiles, pieces = rows // TILE, rows // width
        f32, bf16 = jnp.float32, jnp.bfloat16
        tile3 = (rows // lanes, lanes, num_seeds)
        dma, hbm = pltpu.SemaphoreType.DMA, pl.BlockSpec(memory_space=pl.ANY)
        out = pl.pallas_call(
            functools.partial(sweeps_kernel, n, damping.shape[0], num_nodes),
            out_shape=jax.ShapeDtypeStruct(tile3, f32),
            in_specs=[pl.BlockSpec(memory_space=pltpu.VMEM), pl.BlockSpec(memory_space=pltpu.SMEM), hbm, hbm, hbm],
            out_specs=hbm,
            scratch_shapes=[
                pltpu.VMEM(((n - 2) * pieces, width // TILE, tiles, TILE, TILE), bf16),
                pltpu.VMEM((2, n, HALVES, pieces, num_seeds // HALVES, width), bf16),
                pltpu.VMEM((bufs, tiles, TILE, TILE), bf16),
                pltpu.VMEM(tile3, f32),
                pltpu.VMEM(tile3, f32),
                pltpu.VMEM((num_seeds, lanes), f32),
                pltpu.VMEM((2, n, 8, lanes), f32),
                pltpu.VMEM((num_seeds, lanes), f32),
                dma((2, 8)), dma((2, 8)), dma((2, 4)), dma((2, 8)), dma((2, 8)),
                dma((2,)), dma((2,)), dma((2,)),
                dma(((n - 2) * pieces, width // TILE)), dma((bufs,)), dma((2,)),
            ],
            compiler_params=pltpu.CompilerParams(collective_id=0, has_side_effects=True, vmem_limit_bytes=VMEM_LIMIT),
        )(
            dang_rows.reshape(rows // lanes, lanes),
            damping,
            mat_rows.reshape(tiles, TILE, num_nodes),
            tele_rows.reshape(tile3),
            start_rows.reshape(tile3),
        )
        return out.reshape(rows, num_seeds)

    return jax.shard_map(local_sweeps, mesh=mesh, in_specs=(spec_rows, spec_rows, spec_vec, P(None), spec_rows), out_specs=spec_rows, check_vma=False)
```

```python
import functools

import jax
import jax.numpy as jnp
from jax import lax
from jax.experimental import pallas as pl
from jax.experimental.pallas import tpu as pltpu
from jax.sharding import PartitionSpec as P

MESH = pl.DeviceIdType.MESH
TILE = 256
HALVES = 2
VMEM_LIMIT = 67043328


def product(lhs, rhs, flip):
    return lax.dot_general(lhs, rhs, (((1,), (1 if flip else 0,)), ((), ())), preferred_element_type=jnp.float32)


def sweeps_kernel(n, num_sweeps, num_nodes, dang, damp, a3, e3, r3, out3, cache, gath, stream, et, acc, mcol, pm, part,
                  recv_l, recv_r, sib_own, sib_l, sib_r, send_sem, m_recv, m_send, c_sem, s_sem, io_sem):
    tiles = a3.shape[0]
    pieces, seeds, width = gath.shape[3], gath.shape[4], gath.shape[5]
    kts = width // TILE
    block = pieces * width
    pair = pieces // 2
    chunks = block // TILE
    bufs = stream.shape[0]
    lanes = et.shape[2]
    per_tile = TILE // lanes

    me = lax.axis_index("row")
    step = 1 - 2 * lax.rem(me, 2)
    sib = me + step
    right, left, opp = lax.rem(me + 2, n), lax.rem(me + n - 2, n), lax.rem(me + n // 2, n)

    def piece(slot, blk, h, p, count):
        return gath.at[slot, blk, h, pl.ds(p, count)]

    def remote(slot, blk, h, p, count, recv, dev):
        ref = piece(slot, blk, h, p, count)
        return pltpu.make_async_remote_copy(src_ref=ref, dst_ref=ref, send_sem=send_sem.at[slot], recv_sem=recv,
                                            device_id={"row": dev}, device_id_type=MESH)

    def send(*args):
        remote(*args).start()

    def arrive(slot, blk, h, p, count, recv):
        remote(slot, blk, h, p, count, recv, sib).wait_recv()

    def wait_sends(slot):
        ref = gath.at[slot, pl.ds(0, n - 1)]
        pltpu.make_async_copy(ref, ref, send_sem.at[slot]).wait()

    def others(fn):
        for k in range(1, n):
            fn(lax.rem(me + k, n))

    def stream_copy(c):
        blk = me + (c // chunks) * (sib - me)
        col = pl.multiple_of(blk * block + lax.rem(c, chunks) * TILE, TILE)
        b = lax.rem(c, bufs)
        return pltpu.make_async_copy(a3.at[:, :, pl.ds(col, TILE)], stream.at[b], s_sem.at[b])

    def cache_copy(ci, kt, blk, p):
        col = pl.multiple_of(blk * block + p * width + kt * TILE, TILE)
        return pltpu.make_async_copy(a3.at[:, :, pl.ds(col, TILE)], cache.at[ci, kt], c_sem.at[ci, kt])

    blocks = [left, right, left + step, right + step, opp, opp + step]

    def entry():
        barrier = pltpu.get_barrier_semaphore()
        others(lambda dev: pl.semaphore_signal(barrier, inc=1, device_id={"row": dev}, device_id_type=MESH))
        load_r = pltpu.make_async_copy(r3, acc, io_sem.at[0])
        load_e = pltpu.make_async_copy(e3, et, io_sem.at[1])
        load_r.start()
        load_e.start()
        for c in range(bufs):
            stream_copy(c).start()

        def load_cache():
            def start_cache(b, p):
                for kt in range(kts):
                    cache_copy(b * pieces + p, kt, blocks[b], p).start()

            for i in (1, 0):
                for b in range(4):
                    for j in range(pair):
                        start_cache(b, (i if b % 2 == 0 else 1 - i) * pair + j)
            for b in (4, 5):
                for j in range(pair):
                    start_cache(b, j)
                    start_cache(b, pair + j)

        def send_own(slot, h, u):
            if u == 0:
                send(slot, me, h, 0, pair, recv_l.at[slot, 2 * h], right)
                send(slot, me, h, 0, pair, sib_own.at[slot, 2 * h], sib)
            else:
                send(slot, me, h, pair, pair, recv_r.at[slot, 2 * h], left)
                if h == 0:
                    send_second(slot, h)
                send(slot, me, h, pair, pair, sib_own.at[slot, 2 * h + 1], sib)

        def send_second(slot, h):
            send(slot, me, h, pair, pair, recv_l.at[slot, 2 * h + 1], right)
            send(slot, me, h, 0, pair, recv_r.at[slot, 2 * h + 1], left)

        def pm_copy(slot, dev):
            return pltpu.make_async_remote_copy(src_ref=pm.at[slot, me], dst_ref=pm.at[slot, me], send_sem=m_send.at[slot],
                                                recv_sem=m_recv.at[slot], device_id={"row": dev}, device_id_type=MESH)

        def send_mass(slot):
            mass = jnp.sum(part[...], axis=1, keepdims=True)
            pm[slot, me] = jnp.transpose(jnp.broadcast_to(mass, (HALVES * seeds, lanes)))[: pm.shape[2]]
            others(lambda dev: pm_copy(slot, dev).start())

        def wait_mass(slot):
            ref = pm.at[slot, pl.ds(0, n - 1)]
            pltpu.make_async_copy(ref, ref, m_recv.at[slot]).wait()
            pltpu.make_async_copy(ref, ref, m_send.at[slot]).wait()

        def put(slot, h, j, val):
            p, off = j * lanes // width, j * lanes % width
            gath[slot, me, h, p, :, off : off + lanes] = val.astype(jnp.bfloat16)
            acc[j, h * seeds : (h + 1) * seeds, :] = val
            return val * dang[j : j + 1, :].astype(jnp.float32)

        node_tiles = block // lanes

        load_r.wait()
        pl.semaphore_wait(barrier, n - 1)
        for j in range(node_tiles):
            acc[j] = jnp.transpose(acc[j])
        for h in range(HALVES):
            total = jnp.zeros((seeds, lanes), jnp.float32)
            for j in range(node_tiles):
                total += put(0, h, j, acc[j, h * seeds : (h + 1) * seeds, :])
                if j == node_tiles // 2 - 1:
                    send_own(0, h, 0)
            send_own(0, h, 1)
            part[h * seeds : (h + 1) * seeds, :] = total
        send_mass(0)
        load_e.wait()
        for j in range(node_tiles):
            et[j] = jnp.transpose(et[j])

        def add(i, rows, val, fresh):
            for k in range(per_tile):
                j = i * per_tile + k
                cut = val[:, k * lanes : (k + 1) * lanes]
                acc[j, rows, :] = cut if fresh else acc[j, rows, :] + cut

        def left_side(slot, blk, halves, p, kt):
            cuts = [gath[slot, blk, h, p, :, kt * TILE : (kt + 1) * TILE] for h in halves]
            return cuts[0] if len(cuts) == 1 else jnp.concatenate(cuts, axis=0)

        def compute(first, slot, items, halves):
            rows = slice(halves[0] * seeds, (halves[-1] + 1) * seeds)
            if first:
                for b, p in items:
                    for kt in range(kts):
                        cache_copy(b * pieces + p, kt, blocks[b], p).wait()
            for i in range(tiles):
                val = None
                for b, p in items:
                    for kt in range(kts):
                        rhs = cache[b * pieces + p, kt, i]
                        if first:
                            rhs = jnp.transpose(rhs)
                            cache[b * pieces + p, kt, i] = rhs
                        term = product(left_side(slot, blocks[b], halves, p, kt), rhs, False)
                        val = term if val is None else val + term
                add(i, rows, val, False)

        def near(slot, blk, group):
            rows = slice(0, HALVES * seeds)
            base = group * bufs
            for j in range(bufs):
                c = base + j
                stream_copy(c).wait()
                lhs = left_side(slot, blk, range(HALVES), c % chunks // kts, j % kts)
                for k in range(tiles):
                    add(k, rows, product(lhs, stream[j, k], True), c == 0)
                stream_copy((c + bufs) % (2 * chunks)).start()

        def finish(t, slot, h):
            nxt = 1 - slot
            factor = damp[t]
            rows = slice(h * seeds, (h + 1) * seeds)
            total = jnp.zeros((seeds, lanes), jnp.float32)
            mass = mcol[rows, :] * (factor / num_nodes)
            for i in range(tiles):
                for k in range(per_tile):
                    j = i * per_tile + k
                    val = factor * acc[j, rows, :] + (1.0 - factor) * et[j, rows, :] + mass
                    total += put(nxt, h, j, val)
                if i == tiles // 2 - 1:
                    pl.when(t < num_sweeps - 1)(lambda: send_own(nxt, h, 0))
            pl.when(t < num_sweeps - 1)(lambda: send_own(nxt, h, 1))
            part[rows, :] = total

        def sweep(t, slot, first):
            both = range(HALVES)

            def pass_on(h, i):
                arrive(slot, left, h, i * pair, pair, recv_l.at[slot, 2 * h + i])
                if i == 0:
                    for j in range(pair):
                        send(slot, left, h, j, 1, recv_l.at[slot, 4 + 2 * h + j], right)
                arrive(slot, right, h, (1 - i) * pair, pair, recv_r.at[slot, 2 * h + i])
                if i == 0:
                    for j in range(pair):
                        send(slot, right, h, pair + j, 1, recv_r.at[slot, 4 + 2 * h + j], left)
                    if h == 0:
                        send_second(slot, 1)
                send(slot, left, h, i * pair, pair, sib_l.at[slot, 2 * h + i], sib)
                send(slot, right, h, (1 - i) * pair, pair, sib_r.at[slot, 2 * h + i], sib)

            def pass_far(h, j):
                k = 4 + 2 * h + j
                arrive(slot, opp, h, j, 1, recv_l.at[slot, k])
                send(slot, opp, h, j, 1, sib_l.at[slot, k], sib)
                arrive(slot, opp, h, pair + j, 1, recv_r.at[slot, k])
                send(slot, opp, h, pair + j, 1, sib_r.at[slot, k], sib)

            def around(b, i, halves, turn):
                if b == 2:
                    for h in halves:
                        arrive(slot, blocks[2], h, i * pair, pair, sib_l.at[slot, 2 * h + i])
                        arrive(slot, blocks[3], h, (1 - i) * pair, pair, sib_r.at[slot, 2 * h + i])
                items = [(b + k, (i if k == 0 else 1 - i) * pair + j) for k in range(2) for j in range(pair)]
                compute(turn, slot, items, halves)

            def far(b, h, turn):
                if first:

                    def trip(j, carry):
                        if b == 5:
                            arrive(slot, blocks[5], h, j, 1, sib_l.at[slot, 4 + 2 * h + j])
                            arrive(slot, blocks[5], h, pair + j, 1, sib_r.at[slot, 4 + 2 * h + j])
                        compute(turn, slot, [(b, j), (b, pair + j)], [h])
                        return carry

                    lax.fori_loop(0, pair, trip, 0)
                else:
                    if b == 5:
                        for j in range(pair):
                            arrive(slot, blocks[5], h, j, 1, sib_l.at[slot, 4 + 2 * h + j])
                            arrive(slot, blocks[5], h, pair + j, 1, sib_r.at[slot, 4 + 2 * h + j])
                    compute(turn, slot, [(b, p) for p in range(pieces)], [h])

            near(slot, me, 0)
            if not first:
                wait_sends(1 - slot)
            pass_on(0, 0)
            near(slot, me, 1)
            for h in both:
                for u in range(2):
                    arrive(slot, sib, h, u * pair, pair, sib_own.at[slot, 2 * h + u])
            near(slot, sib, 2)
            pass_on(0, 1)
            near(slot, sib, 3)
            if first:
                load_cache()
            around(0, 1, [0], first)
            pass_on(1, 0)
            around(2, 1, [0], first)
            pass_far(0, 0)
            around(0, 0, both, first)
            pass_far(0, 1)
            around(2, 0, both, first)
            wait_mass(slot)
            row = jnp.sum(pm[slot], axis=0)[0:1]
            mcol[...] = jnp.transpose(jnp.broadcast_to(row, (lanes, HALVES * seeds)))
            far(4, 0, first)
            far(5, 0, first)
            finish(t, slot, 0)
            pass_on(1, 1)
            around(0, 1, [1], False)
            pass_far(1, 0)
            around(2, 1, [1], False)
            pass_far(1, 1)
            far(4, 1, False)
            far(5, 1, False)
            finish(t, slot, 1)
            pl.when(t < num_sweeps - 1)(lambda: send_mass(1 - slot))

        sweep(0, 0, True)

        def trip(t, carry):
            sweep(t, lax.rem(t, 2), False)
            return carry

        lax.fori_loop(1, num_sweeps, trip, 0)

        wait_sends((num_sweeps - 1) % 2)
        for c in range(bufs):
            stream_copy(c).wait()
        for j in range(node_tiles):
            acc[j] = jnp.transpose(acc[j])
        store = pltpu.make_async_copy(acc, out3, io_sem.at[0])
        store.start()
        store.wait()

    entry()


def solution(mesh):
    n = mesh.shape["row"]
    spec_rows = P(("batch", "row"), None)
    spec_vec = P(("batch", "row"))

    def local_sweeps(mat_rows, tele_rows, dang_rows, damping, start_rows):
        rows, num_nodes = mat_rows.shape
        num_seeds = start_rows.shape[1]
        lanes, width, bufs = 128, 512, 4
        assert n == 8 and rows * n == num_nodes and num_seeds == lanes
        tiles, pieces = rows // TILE, rows // width
        f32, bf16 = jnp.float32, jnp.bfloat16
        tile3 = (rows // lanes, lanes, num_seeds)
        dma, hbm = pltpu.SemaphoreType.DMA, pl.BlockSpec(memory_space=pl.ANY)
        out = pl.pallas_call(
            functools.partial(sweeps_kernel, n, damping.shape[0], num_nodes),
            out_shape=jax.ShapeDtypeStruct(tile3, f32),
            in_specs=[pl.BlockSpec(memory_space=pltpu.VMEM), pl.BlockSpec(memory_space=pltpu.SMEM), hbm, hbm, hbm],
            out_specs=hbm,
            scratch_shapes=[
                pltpu.VMEM(((n - 2) * pieces, width // TILE, tiles, TILE, TILE), bf16),
                pltpu.VMEM((2, n, HALVES, pieces, num_seeds // HALVES, width), bf16),
                pltpu.VMEM((bufs, tiles, TILE, TILE), bf16),
                pltpu.VMEM(tile3, f32),
                pltpu.VMEM(tile3, f32),
                pltpu.VMEM((num_seeds, lanes), f32),
                pltpu.VMEM((2, n, 8, lanes), f32),
                pltpu.VMEM((num_seeds, lanes), f32),
                dma((2, 8)), dma((2, 8)), dma((2, 4)), dma((2, 8)), dma((2, 8)),
                dma((2,)), dma((2,)), dma((2,)),
                dma(((n - 2) * pieces, width // TILE)), dma((bufs,)), dma((2,)),
            ],
            compiler_params=pltpu.CompilerParams(collective_id=0, has_side_effects=True, vmem_limit_bytes=VMEM_LIMIT),
        )(
            dang_rows.reshape(rows // lanes, lanes),
            damping,
            mat_rows.reshape(tiles, TILE, num_nodes),
            tele_rows.reshape(tile3),
            start_rows.reshape(tile3),
        )
        return out.reshape(rows, num_seeds)

    return jax.shard_map(local_sweeps, mesh=mesh, in_specs=(spec_rows, spec_rows, spec_vec, P(None), spec_rows), out_specs=spec_rows, check_vma=False)
```

```python
import functools

import jax
import jax.numpy as jnp
from jax import lax
from jax.experimental import pallas as pl
from jax.experimental.pallas import tpu as pltpu
from jax.sharding import PartitionSpec as P

MESH = pl.DeviceIdType.MESH
TILE = 256
HALVES = 2
VMEM_LIMIT = 67043328


def product(lhs, rhs, flip):
    return lax.dot_general(lhs, rhs, (((1,), (1 if flip else 0,)), ((), ())), preferred_element_type=jnp.float32)


def sweeps_kernel(n, num_sweeps, num_nodes, dang, damp, a3, e3, r3, out3, turned, cache, gath, stream, et, acc, mcol, pm, part,
                  recv_l, recv_r, sib_own, sib_l, sib_r, send_sem, m_recv, m_send, c_sem, s_sem, t_sem, io_sem):
    tiles = a3.shape[0]
    pieces, seeds, width = gath.shape[3], gath.shape[4], gath.shape[5]
    kts = width // TILE
    block = pieces * width
    pair = pieces // 2
    chunks = block // TILE
    bufs = stream.shape[0]
    lanes = et.shape[2]
    per_tile = TILE // lanes

    me = lax.axis_index("row")
    step = 1 - 2 * lax.rem(me, 2)
    sib = me + step
    right, left, opp = lax.rem(me + 2, n), lax.rem(me + n - 2, n), lax.rem(me + n // 2, n)

    def piece(slot, blk, h, p, count):
        return gath.at[slot, blk, h, pl.ds(p, count)]

    def remote(slot, blk, h, p, count, recv, dev):
        ref = piece(slot, blk, h, p, count)
        return pltpu.make_async_remote_copy(src_ref=ref, dst_ref=ref, send_sem=send_sem.at[slot], recv_sem=recv,
                                            device_id={"row": dev}, device_id_type=MESH)

    def send(*args):
        remote(*args).start()

    def arrive(slot, blk, h, p, count, recv):
        remote(slot, blk, h, p, count, recv, sib).wait_recv()

    def wait_sends(slot):
        ref = gath.at[slot, pl.ds(0, n - 1)]
        pltpu.make_async_copy(ref, ref, send_sem.at[slot]).wait()

    def others(fn):
        for k in range(1, n):
            fn(lax.rem(me + k, n))

    def stream_copy(c):
        blk = me + (c // chunks) * (sib - me)
        col = pl.multiple_of(blk * block + lax.rem(c, chunks) * TILE, TILE)
        b = lax.rem(c, bufs)
        return pltpu.make_async_copy(a3.at[:, :, pl.ds(col, TILE)], stream.at[b], s_sem.at[b])

    def turned_copy(c):
        b = lax.rem(c, bufs)
        return pltpu.make_async_copy(turned.at[c], stream.at[b], s_sem.at[b])

    def turned_store(c):
        b = lax.rem(c, bufs)
        return pltpu.make_async_copy(stream.at[b], turned.at[c], t_sem.at[b])

    def cache_copy(ci, kt, blk, p):
        col = pl.multiple_of(blk * block + p * width + kt * TILE, TILE)
        return pltpu.make_async_copy(a3.at[:, :, pl.ds(col, TILE)], cache.at[ci, kt], c_sem.at[ci, kt])

    blocks = [left, right, left + step, right + step, opp, opp + step]

    def entry():
        barrier = pltpu.get_barrier_semaphore()
        others(lambda dev: pl.semaphore_signal(barrier, inc=1, device_id={"row": dev}, device_id_type=MESH))
        load_r = pltpu.make_async_copy(r3, acc, io_sem.at[0])
        load_e = pltpu.make_async_copy(e3, et, io_sem.at[1])
        load_r.start()
        load_e.start()
        for c in range(bufs):
            stream_copy(c).start()

        def load_cache():
            def start_cache(b, p):
                for kt in range(kts):
                    cache_copy(b * pieces + p, kt, blocks[b], p).start()

            for i in (1, 0):
                for b in range(4):
                    for j in range(pair):
                        start_cache(b, (i if b % 2 == 0 else 1 - i) * pair + j)
            for b in (4, 5):
                for j in range(pair):
                    start_cache(b, j)
                    start_cache(b, pair + j)

        def send_own(slot, h, u):
            if u == 0:
                send(slot, me, h, 0, pair, recv_l.at[slot, 2 * h], right)
                send(slot, me, h, 0, pair, sib_own.at[slot, 2 * h], sib)
            else:
                send(slot, me, h, pair, pair, recv_r.at[slot, 2 * h], left)
                if h == 0:
                    send_second(slot, h)
                send(slot, me, h, pair, pair, sib_own.at[slot, 2 * h + 1], sib)

        def send_second(slot, h):
            send(slot, me, h, pair, pair, recv_l.at[slot, 2 * h + 1], right)
            send(slot, me, h, 0, pair, recv_r.at[slot, 2 * h + 1], left)

        def pm_copy(slot, dev):
            return pltpu.make_async_remote_copy(src_ref=pm.at[slot, me], dst_ref=pm.at[slot, me], send_sem=m_send.at[slot],
                                                recv_sem=m_recv.at[slot], device_id={"row": dev}, device_id_type=MESH)

        def send_mass(slot):
            mass = jnp.sum(part[...], axis=1, keepdims=True)
            pm[slot, me] = jnp.transpose(jnp.broadcast_to(mass, (HALVES * seeds, lanes)))[: pm.shape[2]]
            others(lambda dev: pm_copy(slot, dev).start())

        def wait_mass(slot):
            ref = pm.at[slot, pl.ds(0, n - 1)]
            pltpu.make_async_copy(ref, ref, m_recv.at[slot]).wait()
            pltpu.make_async_copy(ref, ref, m_send.at[slot]).wait()

        def put(slot, h, j, val):
            p, off = j * lanes // width, j * lanes % width
            gath[slot, me, h, p, :, off : off + lanes] = val.astype(jnp.bfloat16)
            acc[j, h * seeds : (h + 1) * seeds, :] = val
            return val * dang[j : j + 1, :].astype(jnp.float32)

        node_tiles = block // lanes

        load_r.wait()
        pl.semaphore_wait(barrier, n - 1)
        for j in range(node_tiles):
            acc[j] = jnp.transpose(acc[j])
        for h in range(HALVES):
            total = jnp.zeros((seeds, lanes), jnp.float32)
            for j in range(node_tiles):
                total += put(0, h, j, acc[j, h * seeds : (h + 1) * seeds, :])
                if j == node_tiles // 2 - 1:
                    send_own(0, h, 0)
            send_own(0, h, 1)
            part[h * seeds : (h + 1) * seeds, :] = total
        send_mass(0)
        acc[...] = jnp.zeros_like(acc)
        load_e.wait()
        for j in range(node_tiles):
            et[j] = jnp.transpose(et[j])

        def add(i, rows, val, fresh):
            for k in range(per_tile):
                j = i * per_tile + k
                cut = val[:, k * lanes : (k + 1) * lanes]
                acc[j, rows, :] = cut if fresh else acc[j, rows, :] + cut

        def left_side(slot, blk, halves, p, kt):
            cuts = [gath[slot, blk, h, p, :, kt * TILE : (kt + 1) * TILE] for h in halves]
            return cuts[0] if len(cuts) == 1 else jnp.concatenate(cuts, axis=0)

        def compute(first, slot, items, halves):
            rows = slice(halves[0] * seeds, (halves[-1] + 1) * seeds)
            if first:
                for b, p in items:
                    for kt in range(kts):
                        cache_copy(b * pieces + p, kt, blocks[b], p).wait()
            for i in range(tiles):
                val = None
                for b, p in items:
                    for kt in range(kts):
                        rhs = cache[b * pieces + p, kt, i]
                        if first:
                            rhs = jnp.transpose(rhs)
                            cache[b * pieces + p, kt, i] = rhs
                        term = product(left_side(slot, blocks[b], halves, p, kt), rhs, False)
                        val = term if val is None else val + term
                add(i, rows, val, False)

        def near(slot, blk, group):
            rows = slice(0, HALVES * seeds)
            for j in range(bufs):
                c = group * bufs + j
                turned_copy(c).wait()
                lhs = left_side(slot, blk, range(HALVES), c % chunks // kts, j % kts)
                for k in range(tiles):
                    add(k, rows, product(lhs, stream[j, k], False), c == 0)
                turned_copy((c + bufs) % (2 * chunks)).start()

        def release(c):
            turned_store(c).wait()
            pl.when(c + bufs < 2 * chunks)(lambda: stream_copy(c + bufs).start())
            pl.when(c + bufs >= 2 * chunks)(lambda: turned_copy(lax.rem(c + bufs, 2 * chunks)).start())

        def near_first(slot, blk, base):
            rows = slice(0, HALVES * seeds)

            def trip(i, carry):
                for j in range(bufs):
                    c = base + i * bufs + j
                    stream_copy(c).wait()
                    lhs = left_side(slot, blk, range(HALVES), i * (bufs // kts) + j // kts, j % kts)
                    for k in range(tiles):
                        rhs = jnp.transpose(stream[j, k])
                        stream[j, k] = rhs
                        add(k, rows, product(lhs, rhs, False), False)
                    pl.when(c >= 2)(lambda: release(c - 2))
                    turned_store(c).start()
                return carry

            lax.fori_loop(0, chunks // bufs, trip, 0)

        def finish(t, slot, h):
            nxt = 1 - slot
            factor = damp[t]
            rows = slice(h * seeds, (h + 1) * seeds)
            total = jnp.zeros((seeds, lanes), jnp.float32)
            mass = mcol[rows, :] * (factor / num_nodes)
            for i in range(tiles):
                for k in range(per_tile):
                    j = i * per_tile + k
                    val = factor * acc[j, rows, :] + (1.0 - factor) * et[j, rows, :] + mass
                    total += put(nxt, h, j, val)
                if i == tiles // 2 - 1:
                    pl.when(t < num_sweeps - 1)(lambda: send_own(nxt, h, 0))
            pl.when(t < num_sweeps - 1)(lambda: send_own(nxt, h, 1))
            part[rows, :] = total

        def sweep(t, slot, first):
            both = range(HALVES)

            def pass_on(h, i):
                arrive(slot, left, h, i * pair, pair, recv_l.at[slot, 2 * h + i])
                if i == 0:
                    for j in range(pair):
                        send(slot, left, h, j, 1, recv_l.at[slot, 4 + 2 * h + j], right)
                arrive(slot, right, h, (1 - i) * pair, pair, recv_r.at[slot, 2 * h + i])
                if i == 0:
                    for j in range(pair):
                        send(slot, right, h, pair + j, 1, recv_r.at[slot, 4 + 2 * h + j], left)
                    if h == 0:
                        send_second(slot, 1)
                send(slot, left, h, i * pair, pair, sib_l.at[slot, 2 * h + i], sib)
                send(slot, right, h, (1 - i) * pair, pair, sib_r.at[slot, 2 * h + i], sib)

            def pass_far(h, j):
                k = 4 + 2 * h + j
                arrive(slot, opp, h, j, 1, recv_l.at[slot, k])
                send(slot, opp, h, j, 1, sib_l.at[slot, k], sib)
                arrive(slot, opp, h, pair + j, 1, recv_r.at[slot, k])
                send(slot, opp, h, pair + j, 1, sib_r.at[slot, k], sib)

            def around(b, i, halves, turn):
                if b == 2:
                    for h in halves:
                        arrive(slot, blocks[2], h, i * pair, pair, sib_l.at[slot, 2 * h + i])
                        arrive(slot, blocks[3], h, (1 - i) * pair, pair, sib_r.at[slot, 2 * h + i])
                items = [(b + k, (i if k == 0 else 1 - i) * pair + j) for k in range(2) for j in range(pair)]
                compute(turn, slot, items, halves)

            def far(b, h, turn):
                if first:

                    def trip(j, carry):
                        if b == 5:
                            arrive(slot, blocks[5], h, j, 1, sib_l.at[slot, 4 + 2 * h + j])
                            arrive(slot, blocks[5], h, pair + j, 1, sib_r.at[slot, 4 + 2 * h + j])
                        compute(turn, slot, [(b, j), (b, pair + j)], [h])
                        return carry

                    lax.fori_loop(0, pair, trip, 0)
                else:
                    if b == 5:
                        for j in range(pair):
                            arrive(slot, blocks[5], h, j, 1, sib_l.at[slot, 4 + 2 * h + j])
                            arrive(slot, blocks[5], h, pair + j, 1, sib_r.at[slot, 4 + 2 * h + j])
                    compute(turn, slot, [(b, p) for p in range(pieces)], [h])

            if first:
                near_first(slot, me, 0)
            else:
                near(slot, me, 0)
                wait_sends(1 - slot)
            pass_on(0, 0)
            if not first:
                near(slot, me, 1)
            for h in both:
                for u in range(2):
                    arrive(slot, sib, h, u * pair, pair, sib_own.at[slot, 2 * h + u])
            if first:
                near_first(slot, sib, chunks)
            else:
                near(slot, sib, 2)
            pass_on(0, 1)
            if first:
                for c in (2 * chunks - 2, 2 * chunks - 1):
                    release(c)
                load_cache()
            else:
                near(slot, sib, 3)
            around(0, 1, [0], first)
            pass_on(1, 0)
            around(2, 1, [0], first)
            pass_far(0, 0)
            around(0, 0, both, first)
            pass_far(0, 1)
            around(2, 0, both, first)
            wait_mass(slot)
            row = jnp.sum(pm[slot], axis=0)[0:1]
            mcol[...] = jnp.transpose(jnp.broadcast_to(row, (lanes, HALVES * seeds)))
            far(4, 0, first)
            far(5, 0, first)
            finish(t, slot, 0)
            pass_on(1, 1)
            around(0, 1, [1], False)
            pass_far(1, 0)
            around(2, 1, [1], False)
            pass_far(1, 1)
            far(4, 1, False)
            far(5, 1, False)
            finish(t, slot, 1)
            pl.when(t < num_sweeps - 1)(lambda: send_mass(1 - slot))

        sweep(0, 0, True)

        def trip(t, carry):
            sweep(t, lax.rem(t, 2), False)
            return carry

        lax.fori_loop(1, num_sweeps, trip, 0)

        wait_sends((num_sweeps - 1) % 2)
        for c in range(bufs):
            turned_copy(c).wait()
        for j in range(node_tiles):
            acc[j] = jnp.transpose(acc[j])
        store = pltpu.make_async_copy(acc, out3, io_sem.at[0])
        store.start()
        store.wait()

    entry()


def solution(mesh):
    n = mesh.shape["row"]
    spec_rows = P(("batch", "row"), None)
    spec_vec = P(("batch", "row"))

    def local_sweeps(mat_rows, tele_rows, dang_rows, damping, start_rows):
        rows, num_nodes = mat_rows.shape
        num_seeds = start_rows.shape[1]
        lanes, width, bufs = 128, 512, 4
        assert n == 8 and rows * n == num_nodes and num_seeds == lanes
        tiles, pieces = rows // TILE, rows // width
        f32, bf16 = jnp.float32, jnp.bfloat16
        tile3 = (rows // lanes, lanes, num_seeds)
        dma, hbm = pltpu.SemaphoreType.DMA, pl.BlockSpec(memory_space=pl.ANY)
        chunk3 = (2 * rows // TILE, tiles, TILE, TILE)
        out, _ = pl.pallas_call(
            functools.partial(sweeps_kernel, n, damping.shape[0], num_nodes),
            out_shape=(jax.ShapeDtypeStruct(tile3, f32), jax.ShapeDtypeStruct(chunk3, bf16)),
            in_specs=[pl.BlockSpec(memory_space=pltpu.VMEM), pl.BlockSpec(memory_space=pltpu.SMEM), hbm, hbm, hbm],
            out_specs=(hbm, hbm),
            scratch_shapes=[
                pltpu.VMEM(((n - 2) * pieces, width // TILE, tiles, TILE, TILE), bf16),
                pltpu.VMEM((2, n, HALVES, pieces, num_seeds // HALVES, width), bf16),
                pltpu.VMEM((bufs, tiles, TILE, TILE), bf16),
                pltpu.VMEM(tile3, f32),
                pltpu.VMEM(tile3, f32),
                pltpu.VMEM((num_seeds, lanes), f32),
                pltpu.VMEM((2, n, 8, lanes), f32),
                pltpu.VMEM((num_seeds, lanes), f32),
                dma((2, 8)), dma((2, 8)), dma((2, 4)), dma((2, 8)), dma((2, 8)),
                dma((2,)), dma((2,)), dma((2,)),
                dma(((n - 2) * pieces, width // TILE)), dma((bufs,)), dma((bufs,)), dma((2,)),
            ],
            compiler_params=pltpu.CompilerParams(collective_id=0, has_side_effects=True, vmem_limit_bytes=VMEM_LIMIT),
        )(
            dang_rows.reshape(rows // lanes, lanes),
            damping,
            mat_rows.reshape(tiles, TILE, num_nodes),
            tele_rows.reshape(tile3),
            start_rows.reshape(tile3),
        )
        return out.reshape(rows, num_seeds)

    return jax.shard_map(local_sweeps, mesh=mesh, in_specs=(spec_rows, spec_rows, spec_vec, P(None), spec_rows), out_specs=spec_rows, check_vma=False)
```

```python
import functools

import jax
import jax.numpy as jnp
from jax import lax
from jax.experimental import pallas as pl
from jax.experimental.pallas import tpu as pltpu
from jax.sharding import PartitionSpec as P

MESH = pl.DeviceIdType.MESH
TILE = 256
HALVES = 2
VMEM_LIMIT = 67043328


def product(lhs, rhs, flip):
    return lax.dot_general(lhs, rhs, (((1,), (1 if flip else 0,)), ((), ())), preferred_element_type=jnp.float32)


def sweeps_kernel(n, num_sweeps, num_nodes, dang, damp, a3, e3, r3, out3, cache, gath, stream, et, acc, mcol, pm, part,
                  recv_l, recv_r, sib_own, sib_l, sib_r, send_sem, m_recv, m_send, c_sem, s_sem, io_sem):
    tiles = a3.shape[0]
    pieces, seeds, width = gath.shape[3], gath.shape[4], gath.shape[5]
    kts = width // TILE
    block = pieces * width
    pair = pieces // 2
    chunks = block // TILE
    bufs = stream.shape[0]
    lanes = et.shape[2]
    per_tile = TILE // lanes

    me = lax.axis_index("row")
    step = 1 - 2 * lax.rem(me, 2)
    sib = me + step
    right, left, opp = lax.rem(me + 2, n), lax.rem(me + n - 2, n), lax.rem(me + n // 2, n)

    def piece(slot, blk, h, p, count):
        return gath.at[slot, blk, h, pl.ds(p, count)]

    def remote(slot, blk, h, p, count, recv, dev):
        ref = piece(slot, blk, h, p, count)
        return pltpu.make_async_remote_copy(src_ref=ref, dst_ref=ref, send_sem=send_sem.at[slot], recv_sem=recv,
                                            device_id={"row": dev}, device_id_type=MESH)

    def send(*args):
        remote(*args).start()

    def arrive(slot, blk, h, p, count, recv):
        remote(slot, blk, h, p, count, recv, sib).wait_recv()

    def wait_sends(slot):
        ref = gath.at[slot, pl.ds(0, n - 1)]
        pltpu.make_async_copy(ref, ref, send_sem.at[slot]).wait()

    def others(fn):
        for k in range(1, n):
            fn(lax.rem(me + k, n))

    def stream_copy(c):
        blk = me + (c // chunks) * (sib - me)
        col = pl.multiple_of(blk * block + lax.rem(c, chunks) * TILE, TILE)
        b = lax.rem(c, bufs)
        return pltpu.make_async_copy(a3.at[:, :, pl.ds(col, TILE)], stream.at[b], s_sem.at[b])

    def cache_copy(ci, kt, blk, p):
        col = pl.multiple_of(blk * block + p * width + kt * TILE, TILE)
        return pltpu.make_async_copy(a3.at[:, :, pl.ds(col, TILE)], cache.at[ci, kt], c_sem.at[ci, kt])

    blocks = [left, right, left + step, right + step, opp, opp + step]

    def entry():
        barrier = pltpu.get_barrier_semaphore()
        others(lambda dev: pl.semaphore_signal(barrier, inc=1, device_id={"row": dev}, device_id_type=MESH))
        load_r = pltpu.make_async_copy(r3, acc, io_sem.at[0])
        load_e = pltpu.make_async_copy(e3, et, io_sem.at[1])
        load_r.start()
        load_e.start()
        for c in range(bufs):
            stream_copy(c).start()

        def load_cache():
            def start_cache(b, p):
                for kt in range(kts):
                    cache_copy(b * pieces + p, kt, blocks[b], p).start()

            for i in range(2):
                for b in range(4):
                    for j in range(pair):
                        start_cache(b, (i if b % 2 == 0 else 1 - i) * pair + j)
            for b in (4, 5):
                for j in range(pair):
                    start_cache(b, j)
                    start_cache(b, pair + j)

        def send_own(slot, h, u):
            if u == 0:
                send(slot, me, h, 0, pair, recv_l.at[slot, 2 * h], right)
                send(slot, me, h, 0, pair, sib_own.at[slot, 2 * h], sib)
            else:
                send(slot, me, h, pair, pair, recv_r.at[slot, 2 * h], left)
                send(slot, me, h, pair, pair, recv_l.at[slot, 2 * h + 1], right)
                send(slot, me, h, 0, pair, recv_r.at[slot, 2 * h + 1], left)
                send(slot, me, h, pair, pair, sib_own.at[slot, 2 * h + 1], sib)

        def pm_copy(slot, dev):
            return pltpu.make_async_remote_copy(src_ref=pm.at[slot, me], dst_ref=pm.at[slot, me], send_sem=m_send.at[slot],
                                                recv_sem=m_recv.at[slot], device_id={"row": dev}, device_id_type=MESH)

        def send_mass(slot):
            mass = jnp.sum(part[...], axis=1, keepdims=True)
            pm[slot, me] = jnp.transpose(jnp.broadcast_to(mass, (HALVES * seeds, lanes)))[: pm.shape[2]]
            others(lambda dev: pm_copy(slot, dev).start())

        def wait_mass(slot):
            ref = pm.at[slot, pl.ds(0, n - 1)]
            pltpu.make_async_copy(ref, ref, m_recv.at[slot]).wait()
            pltpu.make_async_copy(ref, ref, m_send.at[slot]).wait()

        def put(slot, h, j, val):
            p, off = j * lanes // width, j * lanes % width
            gath[slot, me, h, p, :, off : off + lanes] = val.astype(jnp.bfloat16)
            acc[j, h * seeds : (h + 1) * seeds, :] = val
            return val * dang[j : j + 1, :].astype(jnp.float32)

        node_tiles = block // lanes

        load_r.wait()
        pl.semaphore_wait(barrier, n - 1)
        for j in range(node_tiles):
            acc[j] = jnp.transpose(acc[j])
        for h in range(HALVES):
            total = jnp.zeros((seeds, lanes), jnp.float32)
            for j in range(node_tiles):
                total += put(0, h, j, acc[j, h * seeds : (h + 1) * seeds, :])
                if j == node_tiles // 2 - 1:
                    send_own(0, h, 0)
            send_own(0, h, 1)
            part[h * seeds : (h + 1) * seeds, :] = total
        send_mass(0)
        load_e.wait()
        for j in range(node_tiles):
            et[j] = jnp.transpose(et[j])

        def add(i, rows, val, fresh):
            for k in range(per_tile):
                j = i * per_tile + k
                cut = val[:, k * lanes : (k + 1) * lanes]
                acc[j, rows, :] = cut if fresh else acc[j, rows, :] + cut

        def left_side(slot, blk, halves, p, kt):
            cuts = [gath[slot, blk, h, p, :, kt * TILE : (kt + 1) * TILE] for h in halves]
            return cuts[0] if len(cuts) == 1 else jnp.concatenate(cuts, axis=0)

        def compute(first, slot, items, halves):
            rows = slice(halves[0] * seeds, (halves[-1] + 1) * seeds)
            if first:
                for b, p in items:
                    for kt in range(kts):
                        cache_copy(b * pieces + p, kt, blocks[b], p).wait()
            for i in range(tiles):
                val = None
                for b, p in items:
                    for kt in range(kts):
                        rhs = cache[b * pieces + p, kt, i]
                        if first:
                            rhs = jnp.transpose(rhs)
                            cache[b * pieces + p, kt, i] = rhs
                        term = product(left_side(slot, blocks[b], halves, p, kt), rhs, False)
                        val = term if val is None else val + term
                add(i, rows, val, False)

        def near(slot, blk, base):
            rows = slice(0, HALVES * seeds)

            def chunk(i, j, fresh):
                c = base + i * bufs + j
                p = i * (bufs // kts) + j // kts
                stream_copy(c).wait()
                lhs = left_side(slot, blk, range(HALVES), p, j % kts)
                for k in range(tiles):
                    add(k, rows, product(lhs, stream[j, k], True), fresh)
                stream_copy(lax.rem(c + bufs, 2 * chunks)).start()

            def trip(i, carry):
                for j in range(bufs):
                    chunk(i, j, False)
                return carry

            if base == 0:
                for j in range(bufs):
                    chunk(0, j, j == 0)
            lax.fori_loop(1 if base == 0 else 0, chunks // bufs, trip, 0)

        def finish(t, slot, h):
            nxt = 1 - slot
            factor = damp[t]
            rows = slice(h * seeds, (h + 1) * seeds)
            total = jnp.zeros((seeds, lanes), jnp.float32)
            mass = mcol[rows, :] * (factor / num_nodes)
            for i in range(tiles):
                for k in range(per_tile):
                    j = i * per_tile + k
                    val = factor * acc[j, rows, :] + (1.0 - factor) * et[j, rows, :] + mass
                    total += put(nxt, h, j, val)
                if i == tiles // 2 - 1:
                    pl.when(t < num_sweeps - 1)(lambda: send_own(nxt, h, 0))
            pl.when(t < num_sweeps - 1)(lambda: send_own(nxt, h, 1))
            part[rows, :] = total

        def sweep(t, slot, first):
            near(slot, me, 0)
            for h in range(HALVES):
                for u in range(2):
                    arrive(slot, sib, h, u * pair, pair, sib_own.at[slot, 2 * h + u])
            near(slot, sib, chunks)
            if first:
                load_cache()
            else:
                wait_sends(1 - slot)

            def pass_on(h, i):
                def far_right():
                    for j in range(pair):
                        send(slot, left, h, j, 1, recv_l.at[slot, 4 + 2 * h + j], right)

                def far_left():
                    for j in range(pair):
                        send(slot, right, h, pair + j, 1, recv_r.at[slot, 4 + 2 * h + j], left)

                arrive(slot, left, h, i * pair, pair, recv_l.at[slot, 2 * h + i])
                pl.when(i == 0)(far_right)
                arrive(slot, right, h, (1 - i) * pair, pair, recv_r.at[slot, 2 * h + i])
                pl.when(i == 0)(far_left)
                send(slot, left, h, i * pair, pair, sib_l.at[slot, 2 * h + i], sib)
                send(slot, right, h, (1 - i) * pair, pair, sib_r.at[slot, 2 * h + i], sib)

            pass_on(0, 0)
            pass_on(0, 1)

            def second(i, carry):
                pass_on(1, i)
                compute(first, slot, [(b, (i if b == 0 else 1 - i) * pair + j) for b in (0, 1) for j in range(pair)], range(HALVES))
                for h in range(HALVES):
                    arrive(slot, blocks[2], h, i * pair, pair, sib_l.at[slot, 2 * h + i])
                    arrive(slot, blocks[3], h, (1 - i) * pair, pair, sib_r.at[slot, 2 * h + i])
                compute(first, slot, [(b, (i if b == 2 else 1 - i) * pair + j) for b in (2, 3) for j in range(pair)], range(HALVES))
                return carry

            lax.fori_loop(0, 2, second, 0)
            wait_mass(slot)
            row = jnp.sum(pm[slot], axis=0)[0:1]
            mcol[...] = jnp.transpose(jnp.broadcast_to(row, (lanes, HALVES * seeds)))
            for h in range(HALVES):

                def direct(j, carry):
                    k = 4 + 2 * h + j
                    arrive(slot, opp, h, j, 1, recv_l.at[slot, k])
                    send(slot, opp, h, j, 1, sib_l.at[slot, k], sib)
                    arrive(slot, opp, h, pair + j, 1, recv_r.at[slot, k])
                    send(slot, opp, h, pair + j, 1, sib_r.at[slot, k], sib)
                    compute(first and h == 0, slot, [(4, j), (4, pair + j)], [h])
                    return carry

                lax.fori_loop(0, pair, direct, 0)

                def through(j, carry):
                    k = 4 + 2 * h + j
                    arrive(slot, blocks[5], h, j, 1, sib_l.at[slot, k])
                    arrive(slot, blocks[5], h, pair + j, 1, sib_r.at[slot, k])
                    compute(first and h == 0, slot, [(5, j), (5, pair + j)], [h])
                    return carry

                lax.fori_loop(0, pair, through, 0)
                finish(t, slot, h)
            pl.when(t < num_sweeps - 1)(lambda: send_mass(1 - slot))

        sweep(0, 0, True)

        def trip(t, carry):
            sweep(t, lax.rem(t, 2), False)
            return carry

        lax.fori_loop(1, num_sweeps, trip, 0)

        wait_sends((num_sweeps - 1) % 2)
        for c in range(bufs):
            stream_copy(c).wait()
        for j in range(node_tiles):
            acc[j] = jnp.transpose(acc[j])
        store = pltpu.make_async_copy(acc, out3, io_sem.at[0])
        store.start()
        store.wait()

    entry()


def solution(mesh):
    n = mesh.shape["row"]
    spec_rows = P(("batch", "row"), None)
    spec_vec = P(("batch", "row"))

    def local_sweeps(mat_rows, tele_rows, dang_rows, damping, start_rows):
        rows, num_nodes = mat_rows.shape
        num_seeds = start_rows.shape[1]
        lanes, width, bufs = 128, 512, 4
        assert n == 8 and rows * n == num_nodes and num_seeds == lanes
        tiles, pieces = rows // TILE, rows // width
        f32, bf16 = jnp.float32, jnp.bfloat16
        tile3 = (rows // lanes, lanes, num_seeds)
        dma, hbm = pltpu.SemaphoreType.DMA, pl.BlockSpec(memory_space=pl.ANY)
        out = pl.pallas_call(
            functools.partial(sweeps_kernel, n, damping.shape[0], num_nodes),
            out_shape=jax.ShapeDtypeStruct(tile3, f32),
            in_specs=[pl.BlockSpec(memory_space=pltpu.VMEM), pl.BlockSpec(memory_space=pltpu.SMEM), hbm, hbm, hbm],
            out_specs=hbm,
            scratch_shapes=[
                pltpu.VMEM(((n - 2) * pieces, width // TILE, tiles, TILE, TILE), bf16),
                pltpu.VMEM((2, n, HALVES, pieces, num_seeds // HALVES, width), bf16),
                pltpu.VMEM((bufs, tiles, TILE, TILE), bf16),
                pltpu.VMEM(tile3, f32),
                pltpu.VMEM(tile3, f32),
                pltpu.VMEM((num_seeds, lanes), f32),
                pltpu.VMEM((2, n, 8, lanes), f32),
                pltpu.VMEM((num_seeds, lanes), f32),
                dma((2, 8)), dma((2, 8)), dma((2, 4)), dma((2, 8)), dma((2, 8)),
                dma((2,)), dma((2,)), dma((2,)),
                dma(((n - 2) * pieces, width // TILE)), dma((bufs,)), dma((2,)),
            ],
            compiler_params=pltpu.CompilerParams(collective_id=0, has_side_effects=True, vmem_limit_bytes=VMEM_LIMIT),
        )(
            dang_rows.reshape(rows // lanes, lanes),
            damping,
            mat_rows.reshape(tiles, TILE, num_nodes),
            tele_rows.reshape(tile3),
            start_rows.reshape(tile3),
        )
        return out.reshape(rows, num_seeds)

    return jax.shard_map(local_sweeps, mesh=mesh, in_specs=(spec_rows, spec_rows, spec_vec, P(None), spec_rows), out_specs=spec_rows, check_vma=False)
```
